256 devices in a mesh: grp: 2 (over z), blk: 128 (over y, x, core).
Axes of the slice: x: 8, y: 8, z: 2, core: 2. Of those that a mesh axis runs over, the one named last changes fastest.
The devices are a block of a 8x8x16 slice.
Arguments:
- example_grads: bfloat16 [256, 1048576], P('grp', 'blk'), parts along dimension 0, may hold values from -6 to 6
- tile_seeds: int32 [2048, 8], P('blk'), may hold values from 0 to 16777215
- pair_index: int32 [128, 2], P('grp'), parts along dimension 0, may hold values from 0 to 127
Outputs:
- projected: float32 [4096, 256], P('blk', 'grp'), parts along dimension 1
- scores: float32 [128], P('grp'), parts along dimension 0
The draws below stay inside these ranges and needn't reach their ends.
There are 2 independent parts, one for each index of `grp`. The reference program is written for one: setup_inputs(seed, part) draws one part's arguments, and reference() takes and returns one part's arrays. A program takes and returns all parts, laid end to end along the dimension named above; an argument that names none is the same for every part. Nothing has to cross between parts.
Inputs may be any that keep to these rules, and one draw needn't show every extreme that they name: `pair_index`: column 0 names the query example and column 1 the negative example.
All inputs are finite; a program needn't handle non-finite values.
Results may differ from the reference program's by a relative error of at most 0.0003.
Values sent between devices are 32-bit elements; how exact they have to be, the bound alone decides.
No kernel may reach another device: no remote copies, remote signals or barrier semaphores. Data moves between devices by JAX's collectives and lax.ppermute only.
A program may use at most 64 MiB of HBM per device.

```python
import math
import jax
import jax.numpy as jnp
from jax import lax

K = 4096
TILE = 512
PAIRS = 64
EX = 128
P_SIZE = 1048576


def touch_ends(entries, own_key, least, top_value):
    longest = entries.shape.index(max(entries.shape))
    spots = []
    for shift in (0, 1):
        where = [jax.random.randint(jax.random.fold_in(own_key, axis), (), 0, length) for axis, length in enumerate(entries.shape)]
        where[longest] = (where[longest] + shift) % entries.shape[longest]
        spots.append(tuple(where))
    return entries.at[spots[0]].set(least).at[spots[1]].set(top_value)


def steps_of(key, shape, pieces, least, largest):
    def one(position, blocks):
        heights = jax.random.uniform(jax.random.fold_in(jax.random.fold_in(key, 6), position), (blocks,), jnp.float32, least / len(pieces), largest / len(pieces))
        return jnp.repeat(jnp.exp(heights), shape[position] // blocks).reshape((-1,) + (1,) * (len(shape) - position - 1))

    factor_of = one(*pieces[0])
    for cut in pieces[1:]:
        factor_of = factor_of * one(*cut)
    return factor_of


def normal_values(rng, extent, spread, limit, pieces=(), kind=jnp.bfloat16):
    level = steps_of(rng, extent, pieces, -0.22, 0.18) if pieces else 1.0
    drawn = jax.random.normal(rng, extent, jnp.float32) * spread * level
    return jnp.minimum(jnp.maximum(drawn, -limit), limit).astype(kind)


def setup_inputs(seed: int = 0, part: int = 0) -> dict:
    keys = jax.random.split(jax.random.key(seed), 4)
    own_keys = jax.random.split(jax.random.fold_in(keys[3], part), 4)
    return {
        "example_grads": normal_values(own_keys[0], (EX, P_SIZE), 1.0, 6.0, ((1, 128),)),
        "tile_seeds": touch_ends(jax.random.randint(keys[1], (P_SIZE // TILE, K // TILE), 0, 16777216), jax.random.fold_in(keys[1], 1), 0, 16777215).astype(jnp.int32),
        "pair_index": touch_ends(jax.random.randint(own_keys[2], (PAIRS, 2), 0, EX), jax.random.fold_in(own_keys[2], 1), 0, EX - 1).astype(jnp.int32),
    }


golden_mult = -1640531535
mixer_one = -2048144789
mixer_two = -1028477387

def hashed(seed_value, flat_index):
    mixed = seed_value ^ flat_index * jnp.int32(golden_mult)
    mixed = mixed ^ lax.shift_right_logical(mixed, jnp.int32(16))
    mixed = mixed * jnp.int32(mixer_one)
    mixed = mixed ^ lax.shift_right_logical(mixed, jnp.int32(13))
    mixed = mixed * jnp.int32(mixer_two)
    mixed = mixed ^ lax.shift_right_logical(mixed, jnp.int32(16))
    bit_value = lax.shift_right_logical(mixed, jnp.int32(15)) & jnp.int32(1)
    return jnp.int32(1) - jnp.int32(2) * bit_value

def reference(example_grads, tile_seeds, pair_index):
    examples, params = example_grads.shape
    tile_count = params // TILE
    col_within = jnp.arange(K, dtype=jnp.int32) % TILE
    row_ids = jnp.arange(TILE, dtype=jnp.int32)
    flat_index = row_ids[:, None] * TILE + col_within[None, :]

    def advance(running, tile_pos):
        seed_row = lax.dynamic_index_in_dim(tile_seeds, tile_pos, 0, keepdims=False)
        seed_cols = jnp.broadcast_to(seed_row[:, None], (K // TILE, TILE)).reshape(K)
        sign_tile = hashed(seed_cols[None, :], flat_index).astype(jnp.bfloat16)
        grad_block = lax.dynamic_slice_in_dim(example_grads, tile_pos * TILE, TILE, 1)
        running = running + lax.dot_general(sign_tile, grad_block, (((0,), (1,)), ((), ())), preferred_element_type=jnp.float32)
        return (running, None)
    running, unused = lax.scan(advance, jnp.zeros((K, examples), jnp.float32), jnp.arange(tile_count, dtype=jnp.int32))
    projected = running * (1.0 / math.sqrt(params))
    query_cols = projected[:, pair_index[:, 0]]
    negative_cols = projected[:, pair_index[:, 1]]
    scores = lax.optimization_barrier(jnp.sum(query_cols * negative_cols, axis=0)) * (1.0 / math.sqrt(K))
    return (projected, scores)
```

```python
import functools
import math

import jax
import jax.numpy as jnp
from jax import lax
from jax.experimental import pallas as pl
from jax.experimental.pallas import tpu as pltpu
from jax.sharding import PartitionSpec as P

TILE = 512
PIECE = 16
WIDTH = 256
CORES = 2

golden_mult = -1640531535
mixer_one = -2048144789
mixer_two = -1028477387


def signs(table, seed):
    mixed = (table ^ seed) * jnp.int32(mixer_one)
    mixed = mixed ^ lax.shift_right_logical(mixed, jnp.int32(13))
    mixed = mixed * jnp.int32(mixer_two)
    mixed = mixed ^ lax.shift_right_logical(mixed, jnp.int32(16))
    return jnp.where(mixed.astype(jnp.int16) < 0, jnp.bfloat16(-1), jnp.bfloat16(1))


def project_kernel(own, half, units_ref, seeds_ref, grads_ref, out_ref, table):
    units = units_ref.shape[0]
    tiles = seeds_ref.shape[0]
    examples = grads_ref.shape[0]
    tile_rows = table.shape[0]
    unit_rows = half * tile_rows
    pieces = unit_rows // PIECE
    parts = TILE // WIDTH

    def run(*sums):
        acc = [sums[part * pieces : (part + 1) * pieces] for part in range(parts)]
        for part in range(parts):
            for one in acc[part]:
                pltpu.matmul_pop(one)

        def unit_step(unit, carry):
            x_parity, core, y_parity = units_ref[unit, 0], units_ref[unit, 1], units_ref[unit, 2]
            row = lax.broadcasted_iota(jnp.int32, table.shape, 0)
            param = lax.broadcasted_iota(jnp.int32, table.shape, 1)
            column = ((2 * (row // own) + x_parity) * CORES + core) * own + row % own
            product = (param * TILE + column) * jnp.int32(golden_mult)
            table[...] = product ^ lax.shift_right_logical(product, jnp.int32(16))

            def tile_step(tile, carry):
                for part in range(parts):
                    block = grads_ref[:, pl.ds(pl.multiple_of(tile * TILE + part * WIDTH, WIDTH), WIDTH)]
                    block = jnp.concatenate([block, jnp.zeros((WIDTH - examples, WIDTH), block.dtype)], axis=0)
                    pltpu.matmul_push_rhs(block, staging_register=0, mxu_index=part, transpose=True)
                for i in range(half):
                    seed = seeds_ref[tile, 2 * i + y_parity]
                    seed = seed ^ lax.shift_right_logical(seed, jnp.int32(16))
                    for start in range(0, tile_rows, PIECE):
                        piece = (i * tile_rows + start) // PIECE
                        for part in range(parts):
                            pltpu.matmul_acc_lhs(
                                acc[part][piece],
                                signs(table[start : start + PIECE, part * WIDTH : (part + 1) * WIDTH], seed),
                                load_staged_rhs=0 if piece == 0 else None,
                            )
                return carry

            lax.fori_loop(0, tiles, tile_step, 0)
            for piece in range(pieces):
                total = pltpu.matmul_pop(acc[0][piece])[:, :examples]
                for part in range(1, parts):
                    total = total + pltpu.matmul_pop(acc[part][piece])[:, :examples]
                out_ref[pl.ds(pl.multiple_of(unit * unit_rows + piece * PIECE, PIECE), PIECE), :] = total
            return carry

        lax.fori_loop(0, units, unit_step, 0)

    pl.run_scoped(run, *[pltpu.ACC(part)((PIECE, WIDTH), jnp.float32) for part in range(parts) for _ in range(pieces)])


def project(units, seeds, grads, own, side):
    examples, params = grads.shape
    half = side // 2
    tile_rows = half * own
    rows = units.shape[0] * half * tile_rows
    return pl.pallas_call(
        functools.partial(project_kernel, own, half),
        out_shape=jax.ShapeDtypeStruct((rows, examples), jnp.float32),
        in_specs=[
            pl.BlockSpec(memory_space=pltpu.SMEM),
            pl.BlockSpec(memory_space=pltpu.SMEM),
            pl.BlockSpec(memory_space=pltpu.VMEM),
        ],
        out_specs=pl.BlockSpec(memory_space=pltpu.VMEM),
        scratch_shapes=[pltpu.VMEM((tile_rows, TILE), jnp.int32)],
        compiler_params=pltpu.CompilerParams(vmem_limit_bytes=12 << 20),
        cost_estimate=pl.CostEstimate(
            flops=8 * rows * examples * params, bytes_accessed=2 * examples * params, transcendentals=0
        ),
        name="project",
    )(units, seeds, grads)


def finish_kernel(scaling, parts_ref, pairs_ref, own_ref, score_ref):
    total = parts_ref[0]
    for k in range(1, parts_ref.shape[0]):
        total = total + parts_ref[k]
    total = total * jnp.float32(scaling)
    own_ref[...] = total
    examples = total.shape[1]
    ids = lax.broadcasted_iota(jnp.int32, (examples, pairs_ref.shape[1]), 0)

    def pick(which):
        chosen = (ids == pairs_ref[which : which + 1, :]).astype(jnp.float32)
        return jnp.dot(total, chosen, precision=lax.Precision.HIGHEST, preferred_element_type=jnp.float32)

    score_ref[...] = jnp.sum(pick(0) * pick(1), axis=0, keepdims=True)


def finish(parts, pairs, scaling):
    vmem = pl.BlockSpec(memory_space=pltpu.VMEM)
    return pl.pallas_call(
        functools.partial(finish_kernel, scaling),
        out_shape=(
            jax.ShapeDtypeStruct(parts.shape[1:], jnp.float32),
            jax.ShapeDtypeStruct((1, pairs.shape[1]), jnp.float32),
        ),
        in_specs=[vmem, vmem],
        out_specs=(vmem, vmem),
        compiler_params=pltpu.CompilerParams(vmem_limit_bytes=12 << 20),
        name="finish",
    )(parts, pairs)


def per_device(example_grads, tile_seeds, pair_index):
    examples, params = example_grads.shape
    devices = lax.axis_size("blk")
    col_total = tile_seeds.shape[1] * TILE
    own = col_total // devices
    side = math.isqrt(devices // CORES)
    half = side // 2
    assert side * side * CORES == devices and side * CORES * own == TILE
    me = lax.axis_index("blk")
    core = me % CORES

    def place(y, x, c):
        return (y * side + x) * CORES + c

    order = [(px, py, i, j) for px in range(2) for py in range(2) for i in range(half) for j in range(half)]
    chips = [[place(2 * i + py, 2 * j + px, c) for px, py, i, j in order] for c in range(CORES)]
    partner = [(d, d ^ 1) for d in range(devices)]

    def units(which_core):
        return jnp.stack([jnp.stack([jnp.int32(px), which_core, jnp.int32(py)]) for px in range(2) for py in range(2)])

    theirs = project(units(1 - core), tile_seeds, example_grads, own, side)
    received = lax.ppermute(theirs, "blk", partner)
    mine = project(units(core), tile_seeds, example_grads, own, side)
    both = (mine + received).reshape(side * side, own, examples)
    parts = lax.all_to_all(both, "blk", 0, 0, axis_index_groups=chips, tiled=True)
    own_rows, partial = finish(parts, pair_index.T, 1.0 / math.sqrt(params * devices))
    partial = partial + lax.ppermute(partial, "blk", partner)
    spread = jnp.broadcast_to(partial[None], (side * side,) + partial.shape)
    shares = lax.all_to_all(spread, "blk", 0, 0, axis_index_groups=chips, tiled=True)
    scores = jnp.sum(shares, axis=(0, 1)) * (1.0 / math.sqrt(col_total))
    return (own_rows, scores)


def solution(mesh):
    placed = (P("grp", "blk"), P("blk", None), P("grp", None))
    return jax.shard_map(
        per_device,
        mesh=mesh,
        in_specs=placed,
        out_specs=(P("blk", "grp"), P("grp")),
        check_vma=False,
    )
```

```python
import functools
import math

import jax
import jax.numpy as jnp
from jax import lax
from jax.experimental import pallas as pl
from jax.experimental.pallas import tpu as pltpu
from jax.sharding import PartitionSpec as P

TILE = 512
PIECE = 16
WIDTH = 256
CORES = 2

golden_mult = -1640531535
mixer_one = -2048144789
mixer_two = -1028477387


def signs(table, seed):
    mixed = (table ^ seed) * jnp.int32(mixer_one)
    mixed = mixed ^ lax.shift_right_logical(mixed, jnp.int32(13))
    mixed = mixed * jnp.int32(mixer_two)
    mixed = mixed ^ lax.shift_right_logical(mixed, jnp.int32(16))
    return jnp.where(mixed.astype(jnp.int16) < 0, jnp.bfloat16(-1), jnp.bfloat16(1))


def project_kernel(own, half, side, units, flips, me_ref, seeds_ref, grads_ref, out_ref, table):
    me = me_ref[0]
    own_core = me & (CORES - 1)
    own_x = (me // CORES) & 1
    own_y = (me // (CORES * side)) & 1
    x_flip, y_flip, core_flip = flips
    x_parity, core = own_x ^ x_flip, own_core ^ core_flip
    tiles = seeds_ref.shape[0]
    examples = grads_ref.shape[0]
    tile_rows = table.shape[0]
    unit_rows = half * tile_rows
    pieces = unit_rows // PIECE
    parts = TILE // WIDTH

    def run(*sums):
        acc = [sums[part * pieces : (part + 1) * pieces] for part in range(parts)]
        for part in range(parts):
            for one in acc[part]:
                pltpu.matmul_pop(one)

        row = lax.broadcasted_iota(jnp.int32, table.shape, 0)
        param = lax.broadcasted_iota(jnp.int32, table.shape, 1)
        column = ((2 * (row // own) + x_parity) * CORES + core) * own + row % own
        product = (param * TILE + column) * jnp.int32(golden_mult)
        table[...] = product ^ lax.shift_right_logical(product, jnp.int32(16))

        def unit_step(unit, carry):
            y_parity = own_y ^ y_flip ^ (unit & 1)
            def tile_step(tile, carry):
                for part in range(parts):
                    block = grads_ref[:, pl.ds(pl.multiple_of(tile * TILE + part * WIDTH, WIDTH), WIDTH)]
                    block = jnp.concatenate([block, jnp.zeros((WIDTH - examples, WIDTH), block.dtype)], axis=0)
                    pltpu.matmul_push_rhs(block, staging_register=0, mxu_index=part, transpose=True)
                for i in range(half):
                    seed = seeds_ref[tile, 2 * i + y_parity]
                    seed = seed ^ lax.shift_right_logical(seed, jnp.int32(16))
                    for start in range(0, tile_rows, PIECE):
                        piece = (i * tile_rows + start) // PIECE
                        for part in range(parts):
                            pltpu.matmul_acc_lhs(
                                acc[part][piece],
                                signs(table[start : start + PIECE, part * WIDTH : (part + 1) * WIDTH], seed),
                                load_staged_rhs=0 if piece == 0 else None,
                            )
                return carry

            lax.fori_loop(0, tiles, tile_step, 0)
            for piece in range(pieces):
                total = pltpu.matmul_pop(acc[0][piece])[:, :examples]
                for part in range(1, parts):
                    total = total + pltpu.matmul_pop(acc[part][piece])[:, :examples]
                out_ref[pl.ds(pl.multiple_of(unit * unit_rows + piece * PIECE, PIECE), PIECE), :] = total
            return carry

        lax.fori_loop(0, units, unit_step, 0)

    pl.run_scoped(run, *[pltpu.ACC(part)((PIECE, WIDTH), jnp.float32) for part in range(parts) for _ in range(pieces)])


def project(me, seeds, grads, own, side, units, flips):
    examples, params = grads.shape
    half = side // 2
    tile_rows = half * own
    rows = units * half * tile_rows
    return pl.pallas_call(
        functools.partial(project_kernel, own, half, side, units, flips),
        out_shape=jax.ShapeDtypeStruct((rows, examples), jnp.float32),
        in_specs=[
            pl.BlockSpec(memory_space=pltpu.SMEM),
            pl.BlockSpec(memory_space=pltpu.SMEM),
            pl.BlockSpec(memory_space=pltpu.VMEM),
        ],
        out_specs=pl.BlockSpec(memory_space=pltpu.VMEM),
        scratch_shapes=[pltpu.VMEM((tile_rows, TILE), jnp.int32)],
        compiler_params=pltpu.CompilerParams(vmem_limit_bytes=12 << 20),
        cost_estimate=pl.CostEstimate(
            flops=8 * rows * examples * params, bytes_accessed=2 * examples * params, transcendentals=0
        ),
        name="project",
    )(me, seeds, grads)


def finish_kernel(scaling, parts_ref, pairs_ref, own_ref, score_ref):
    total = parts_ref[0]
    for k in range(1, parts_ref.shape[0]):
        total = total + parts_ref[k]
    total = total * jnp.float32(scaling)
    own_ref[...] = total
    examples = total.shape[1]
    ids = lax.broadcasted_iota(jnp.int32, (examples, pairs_ref.shape[1]), 0)

    def pick(which):
        chosen = (ids == pairs_ref[which : which + 1, :]).astype(jnp.float32)
        return jnp.dot(total, chosen, precision=lax.Precision.HIGHEST, preferred_element_type=jnp.float32)

    score_ref[...] = jnp.sum(pick(0) * pick(1), axis=0, keepdims=True)


def finish(parts, pairs, scaling):
    vmem = pl.BlockSpec(memory_space=pltpu.VMEM)
    return pl.pallas_call(
        functools.partial(finish_kernel, scaling),
        out_shape=(
            jax.ShapeDtypeStruct(parts.shape[1:], jnp.float32),
            jax.ShapeDtypeStruct((1, pairs.shape[1]), jnp.float32),
        ),
        in_specs=[vmem, vmem],
        out_specs=(vmem, vmem),
        compiler_params=pltpu.CompilerParams(vmem_limit_bytes=12 << 20),
        name="finish",
    )(parts, pairs)


def per_device(example_grads, tile_seeds, pair_index):
    examples, params = example_grads.shape
    devices = lax.axis_size("blk")
    col_total = tile_seeds.shape[1] * TILE
    own = col_total // devices
    side = math.isqrt(devices // CORES)
    half = side // 2
    assert side * side * CORES == devices and side * CORES * own == TILE and side % 2 == 0
    me = lax.axis_index("blk").astype(jnp.int32).reshape(1)

    def place(y, x, c):
        return (y * side + x) * CORES + c

    def swap(array, flip):
        return lax.ppermute(array, "blk", [(d, d ^ flip) for d in range(devices)])

    def columns(units, x_flip, y_flip, core_flip):
        return project(me, tile_seeds, example_grads, own, side, units, (x_flip, y_flip, core_flip))

    alike = [
        [place(2 * i + py, 2 * j + px, c) for i in range(half) for j in range(half)]
        for py in range(2)
        for px in range(2)
        for c in range(CORES)
    ]
    chips = [[place(y, x, c) for y in range(side) for x in range(side)] for c in range(CORES)]
    next_core, next_x, next_y = 1, CORES, CORES * side
    middle = half * half * own

    other_x = swap(columns(2, 1, 1, 1), next_core) + columns(2, 1, 1, 0)
    other_x = swap(other_x, next_x)
    other_y = swap(columns(1, 0, 1, 1), next_core) + columns(1, 0, 1, 0) + other_x[:middle]
    other_y = swap(other_y, next_y)
    same = swap(columns(1, 0, 0, 1), next_core) + columns(1, 0, 0, 0) + other_x[middle:] + other_y
    parts = lax.all_to_all(same.reshape(half * half, own, examples), "blk", 0, 0, axis_index_groups=alike, tiled=True)
    own_rows, partial = finish(parts, pair_index.T, 1.0 / math.sqrt(params * devices))
    partial = partial + swap(partial, next_core)
    spread = jnp.broadcast_to(partial[None], (side * side,) + partial.shape)
    shares = lax.all_to_all(spread, "blk", 0, 0, axis_index_groups=chips, tiled=True)
    scores = jnp.sum(shares, axis=(0, 1)) * (1.0 / math.sqrt(col_total))
    return (own_rows, scores)


def solution(mesh):
    placed = (P("grp", "blk"), P("blk", None), P("grp", None))
    return jax.shard_map(
        per_device,
        mesh=mesh,
        in_specs=placed,
        out_specs=(P("blk", "grp"), P("grp")),
        check_vma=False,
    )
```

```python
import functools
import math

import jax
import jax.numpy as jnp
from jax import lax
from jax.experimental import pallas as pl
from jax.experimental.pallas import tpu as pltpu
from jax.sharding import PartitionSpec as P


TILE = 512
PIECE = 16
WIDTH = 256
CORES = 2

golden_mult = -1640531535
mixer_one = -2048144789
mixer_two = -1028477387


def signs(table, seed):
    mixed = (table ^ seed) * jnp.int32(mixer_one)
    mixed = mixed ^ lax.shift_right_logical(mixed, jnp.int32(13))
    mixed = mixed * jnp.int32(mixer_two)
    mixed = mixed ^ lax.shift_right_logical(mixed, jnp.int32(16))
    return jnp.where(mixed.astype(jnp.int16) < 0, jnp.bfloat16(-1), jnp.bfloat16(1))


def prepare_kernel(half, side, me_ref, seeds_ref, rows_ref):
    tiles = seeds_ref.shape[0]
    me = me_ref[0]
    own_y = (me // (CORES * side)) & 1
    last = 2 * half * tiles
    rows_ref[last:, :] = jnp.full((rows_ref.shape[0] - last, WIDTH), me & (2 * CORES - 1), jnp.int32)
    seeds = seeds_ref[...]
    seeds = seeds ^ lax.shift_right_logical(seeds, jnp.int32(16))
    for y in range(2 * half):
        row = pl.multiple_of((((y & 1) ^ own_y) * half + y // 2) * tiles, tiles)
        rows_ref[pl.ds(row, tiles), :] = jnp.broadcast_to(seeds[:, y : y + 1], (tiles, WIDTH))


def prepare(me, seeds, side):
    half = side // 2
    vmem = pl.BlockSpec(memory_space=pltpu.VMEM)
    return pl.pallas_call(
        functools.partial(prepare_kernel, half, side),
        out_shape=jax.ShapeDtypeStruct((2 * seeds.shape[0] * half + 8, WIDTH), jnp.int32),
        in_specs=[pl.BlockSpec(memory_space=pltpu.SMEM), vmem],
        out_specs=vmem,
        compiler_params=pltpu.CompilerParams(vmem_limit_bytes=12 << 20),
        cost_estimate=pl.CostEstimate(flops=1 << 30, bytes_accessed=1 << 16, transcendentals=0),
        name="prepare",
    )(me, seeds)


def project_kernel(own, half, tiles, flips, after_ref, seeds_ref, grads_ref, out_ref, table):
    del after_ref
    x_flip, y_flip, core_flip = flips
    examples = grads_ref.shape[0]
    tile_rows = table.shape[0]
    unit_rows = half * tile_rows
    pieces = unit_rows // PIECE
    parts = TILE // WIDTH

    def run(*sums):
        acc = [sums[part * pieces : (part + 1) * pieces] for part in range(parts)]
        for part in range(parts):
            for one in acc[part]:
                pltpu.matmul_pop(one)
        place = seeds_ref[2 * tiles * half : 2 * tiles * half + 1, :] ^ (x_flip * CORES + core_flip)
        row = lax.broadcasted_iota(jnp.int32, (tile_rows, WIDTH), 0)
        column = (row // own) * (2 * CORES * own) + row % own + place * own
        for start in range(0, TILE, WIDTH):
            param = lax.broadcasted_iota(jnp.int32, (tile_rows, WIDTH), 1) + start
            product = (param * TILE + column) * jnp.int32(golden_mult)
            table[:, start : start + WIDTH] = product ^ lax.shift_right_logical(product, jnp.int32(16))

        def push(tile):
            for part in range(parts):
                block = grads_ref[:, pl.ds(pl.multiple_of(tile * TILE + part * WIDTH, WIDTH), WIDTH)]
                block = jnp.concatenate([block, jnp.zeros((WIDTH - examples, WIDTH), block.dtype)], axis=0)
                pltpu.matmul_push_rhs(block, staging_register=0, mxu_index=part, transpose=True)

        def tile_step(first_seed, tile, following):
            for i in range(half):
                seed = seeds_ref[pl.ds(first_seed + i * tiles + tile, 1), :]
                for start in range(0, tile_rows, PIECE):
                    piece = (i * tile_rows + start) // PIECE
                    for part in range(parts):
                        pltpu.matmul_acc_lhs(
                            acc[part][piece],
                            signs(table[start : start + PIECE, part * WIDTH : (part + 1) * WIDTH], seed),
                            load_staged_rhs=0 if piece == 0 else None,
                        )
                    if piece == 0 and following is not None:
                        push(following)

        first_seed = y_flip * half * tiles
        push(0)

        def pair_step(pair, carry):
            tile_step(first_seed, 2 * pair, 2 * pair + 1)
            tile_step(first_seed, 2 * pair + 1, 2 * pair + 2)
            return carry

        lax.fori_loop(0, tiles // 2 - 1, pair_step, 0)
        tile_step(first_seed, tiles - 2, tiles - 1)
        tile_step(first_seed, tiles - 1, None)
        for piece in range(pieces):
            total = pltpu.matmul_pop(acc[0][piece])[:, :examples]
            for part in range(1, parts):
                total = total + pltpu.matmul_pop(acc[part][piece])[:, :examples]
            out_ref[piece * PIECE : (piece + 1) * PIECE, :] = total

    pl.run_scoped(run, *[pltpu.ACC(part)((PIECE, WIDTH), jnp.float32) for part in range(parts) for _ in range(pieces)])


def project(after, seeds, grads, own, side, flips):
    examples, params = grads.shape
    half = side // 2
    tile_rows = half * own
    rows = half * tile_rows
    vmem = pl.BlockSpec(memory_space=pltpu.VMEM)
    return pl.pallas_call(
        functools.partial(project_kernel, own, half, params // TILE, flips),
        out_shape=jax.ShapeDtypeStruct((rows, examples), jnp.float32),
        in_specs=[vmem, vmem, vmem],
        out_specs=vmem,
        scratch_shapes=[pltpu.VMEM((tile_rows, TILE), jnp.int32)],
        compiler_params=pltpu.CompilerParams(vmem_limit_bytes=12 << 20),
        cost_estimate=pl.CostEstimate(
            flops=8 * rows * examples * params, bytes_accessed=2 * examples * params, transcendentals=0
        ),
        name="project",
    )(after, seeds, grads)


def finish_kernel(scaling, score_scaling, parts_ref, pairs_ref, own_ref, score_ref):
    total = parts_ref[0]
    for k in range(1, parts_ref.shape[0]):
        total = total + parts_ref[k]
    total = total * jnp.float32(scaling)
    own_ref[...] = total
    examples = total.shape[1]
    ids = lax.broadcasted_iota(jnp.int32, (examples, pairs_ref.shape[1]), 0)

    def pick(which):
        chosen = (ids == pairs_ref[which : which + 1, :]).astype(jnp.float32)
        return jnp.dot(total, chosen, precision=lax.Precision.HIGHEST, preferred_element_type=jnp.float32)

    score_ref[...] = jnp.sum(pick(0) * pick(1), axis=0, keepdims=True) * jnp.float32(score_scaling)


def finish(parts, pairs, scaling, score_scaling):
    vmem = pl.BlockSpec(memory_space=pltpu.VMEM)
    return pl.pallas_call(
        functools.partial(finish_kernel, scaling, score_scaling),
        out_shape=(
            jax.ShapeDtypeStruct(parts.shape[1:], jnp.float32),
            jax.ShapeDtypeStruct((1, pairs.shape[1]), jnp.float32),
        ),
        in_specs=[vmem, vmem],
        out_specs=(vmem, vmem),
        compiler_params=pltpu.CompilerParams(vmem_limit_bytes=12 << 20),
        name="finish",
    )(parts, pairs)


def per_device(example_grads, tile_seeds, pair_index):
    examples, params = example_grads.shape
    devices = lax.axis_size("blk")
    col_total = tile_seeds.shape[1] * TILE
    own = col_total // devices
    side = math.isqrt(devices // CORES)
    half = side // 2
    assert side * side * CORES == devices and side * CORES * own == TILE and side % 2 == 0
    me = lax.axis_index("blk").astype(jnp.int32).reshape(1)

    def place(y, x, c):
        return (y * side + x) * CORES + c

    def swap(array, flip):
        return lax.ppermute(array, "blk", [(d, d ^ flip) for d in range(devices)])

    seeds = prepare(me, tile_seeds, side)

    alike = [
        [place(2 * i + py, 2 * j + px, c) for i in range(half) for j in range(half)]
        for py in range(2)
        for px in range(2)
        for c in range(CORES)
    ]
    chips = [[place(y, x, c) for y in range(side) for x in range(side)] for c in range(CORES)]
    next_core, next_x, next_y = 1, CORES, CORES * side

    def columns(after, x_flip, y_flip, core_flip):
        return project(after, seeds, example_grads, own, side, (x_flip, y_flip, core_flip))

    both_far = columns(seeds, 1, 1, 1)
    x_far = columns(both_far, 1, 0, 1)
    both = columns(x_far, 1, 1, 0) + swap(both_far, next_core)
    both_in = swap(both, next_x)
    x_own = columns(both, 1, 0, 0) + swap(x_far, next_core)
    x_in = swap(x_own, next_x)
    y_far = columns(x_own, 0, 1, 1)
    y_own = columns(y_far, 0, 1, 0) + swap(y_far, next_core) + both_in
    y_in = swap(y_own, next_y)
    far = columns(y_own, 0, 0, 1)
    same = columns(far, 0, 0, 0) + swap(far, next_core) + x_in + y_in
    parts = lax.all_to_all(same.reshape(half * half, own, examples), "blk", 0, 0, axis_index_groups=alike, tiled=True)
    own_rows, partial = finish(parts, pair_index.T, 1.0 / math.sqrt(params * devices), 1.0 / math.sqrt(col_total))
    partial = partial + swap(partial, next_core)
    spread = jnp.broadcast_to(partial[None], (side * side,) + partial.shape)
    shares = lax.all_to_all(spread, "blk", 0, 0, axis_index_groups=chips, tiled=True)
    scores = jnp.sum(shares, axis=(0, 1))
    return (own_rows, scores)


def solution(mesh):
    placed = (P("grp", "blk"), P("blk", None), P("grp", None))
    return jax.shard_map(
        per_device,
        mesh=mesh,
        in_specs=placed,
        out_specs=(P("blk", "grp"), P("grp")),
        check_vma=False,
    )
```

```python
import functools
import math

import jax
import jax.numpy as jnp
from jax import lax
from jax.experimental import pallas as pl
from jax.experimental.pallas import tpu as pltpu
from jax.sharding import PartitionSpec as P


TILE = 512
PIECE = 16
WIDTH = 256
CORES = 2

golden_mult = -1640531535
mixer_one = -2048144789
mixer_two = -1028477387


def minus_two_bits(table, seed):
    mixed = (table ^ seed) * jnp.int32(mixer_one)
    mixed = mixed ^ lax.shift_right_logical(mixed, jnp.int32(13))
    mixed = mixed * jnp.int32(mixer_two)
    mixed = mixed ^ lax.shift_right_logical(mixed, jnp.int32(16))
    return jnp.where(mixed.astype(jnp.int16) < 0, jnp.bfloat16(-2), jnp.bfloat16(0))


def prepare_kernel(half, side, own, me_ref, seeds_ref, rows_ref, tables_ref):
    tiles = seeds_ref.shape[0]
    me = me_ref[0]
    own_y = (me // (CORES * side)) & 1
    shape = (half * own, TILE)
    row = lax.broadcasted_iota(jnp.int32, shape, 0)
    param = lax.broadcasted_iota(jnp.int32, shape, 1)
    index = param * TILE + (row // own) * (2 * CORES * own) + row % own
    for flip in range(2 * CORES):
        place = (me & (2 * CORES - 1)) ^ flip
        product = (index + place * own) * jnp.int32(golden_mult)
        tables_ref[flip * half * own : (flip + 1) * half * own, :] = product ^ lax.shift_right_logical(product, jnp.int32(16))
    seeds = seeds_ref[...]
    seeds = seeds ^ lax.shift_right_logical(seeds, jnp.int32(16))
    for y in range(2 * half):
        row = pl.multiple_of((((y & 1) ^ own_y) * half + y // 2) * tiles, tiles)
        rows_ref[pl.ds(row, tiles), :] = jnp.broadcast_to(seeds[:, y : y + 1], (tiles, WIDTH))


def prepare(me, seeds, side, own):
    half = side // 2
    vmem = pl.BlockSpec(memory_space=pltpu.VMEM)
    return pl.pallas_call(
        functools.partial(prepare_kernel, half, side, own),
        out_shape=(
            jax.ShapeDtypeStruct((2 * half * seeds.shape[0], WIDTH), jnp.int32),
            jax.ShapeDtypeStruct((2 * CORES * half * own, TILE), jnp.int32),
        ),
        in_specs=[pl.BlockSpec(memory_space=pltpu.SMEM), vmem],
        out_specs=(vmem, vmem),
        compiler_params=pltpu.CompilerParams(vmem_limit_bytes=12 << 20),
        cost_estimate=pl.CostEstimate(flops=1 << 30, bytes_accessed=1 << 16, transcendentals=0),
        name="prepare",
    )(me, seeds)


def project_kernel(own, half, tiles, flips, first, after_ref, seeds_ref, tables_ref, grads_ref, out_ref):
    del after_ref
    x_flip, y_flip, core_flip = flips
    examples = grads_ref.shape[0]
    tile_rows = half * own
    table = tables_ref.at[(x_flip * CORES + core_flip) * tile_rows : (x_flip * CORES + core_flip + 1) * tile_rows, :]
    pieces = half * tile_rows // PIECE
    parts = TILE // WIDTH

    def run(*sums):
        acc = [sums[part * (pieces + 1) : (part + 1) * (pieces + 1)] for part in range(parts)]
        if first:
            for one in sums:
                pltpu.matmul_pop(one)

        def push(tile):
            for part in range(parts):
                block = grads_ref[:, pl.ds(pl.multiple_of(tile * TILE + part * WIDTH, WIDTH), WIDTH)]
                block = jnp.concatenate([block, jnp.zeros((WIDTH - examples, WIDTH), block.dtype)], axis=0)
                pltpu.matmul_push_rhs(block, staging_register=0, mxu_index=part, transpose=True)

        def tile_step(first_seed, tile, following):
            for part in range(parts):
                pltpu.matmul_acc_lhs(acc[part][pieces], jnp.ones((PIECE, WIDTH), jnp.bfloat16), load_staged_rhs=0)
            if following is not None:
                push(following)
            for i in range(half):
                seed = seeds_ref[pl.ds(first_seed + i * tiles + tile, 1), :]
                for start in range(0, tile_rows, PIECE):
                    piece = (i * tile_rows + start) // PIECE
                    for part in range(parts):
                        pltpu.matmul_acc_lhs(
                            acc[part][piece],
                            minus_two_bits(table[start : start + PIECE, part * WIDTH : (part + 1) * WIDTH], seed),
                        )

        first_seed = y_flip * half * tiles
        push(0)

        def pair_step(pair, carry):
            tile_step(first_seed, 2 * pair, 2 * pair + 1)
            tile_step(first_seed, 2 * pair + 1, 2 * pair + 2)
            return carry

        lax.fori_loop(0, tiles // 2 - 1, pair_step, 0)
        tile_step(first_seed, tiles - 2, tiles - 1)
        tile_step(first_seed, tiles - 1, None)
        whole = sum(pltpu.matmul_pop(acc[part][pieces])[:, :examples] for part in range(parts))
        for piece in range(pieces):
            total = sum(pltpu.matmul_pop(acc[part][piece])[:, :examples] for part in range(parts))
            out_ref[piece * PIECE : (piece + 1) * PIECE, :] = whole + total

    pl.run_scoped(run, *[pltpu.ACC(part)((PIECE, WIDTH), jnp.float32) for part in range(parts) for _ in range(pieces + 1)])


def project(after, seeds, tables, grads, own, side, flips):
    examples, params = grads.shape
    half = side // 2
    tile_rows = half * own
    rows = half * tile_rows
    vmem = pl.BlockSpec(memory_space=pltpu.VMEM)
    return pl.pallas_call(
        functools.partial(project_kernel, own, half, params // TILE, flips, after is seeds),
        out_shape=jax.ShapeDtypeStruct((rows, examples), jnp.float32),
        in_specs=[vmem] * 4,
        out_specs=vmem,
        compiler_params=pltpu.CompilerParams(vmem_limit_bytes=12 << 20),
        cost_estimate=pl.CostEstimate(
            flops=8 * rows * examples * params, bytes_accessed=2 * examples * params, transcendentals=0
        ),
        name="project",
    )(after, seeds, tables, grads)


def finish_kernel(scaling, score_scaling, parts_ref, pairs_ref, own_ref, score_ref):
    total = parts_ref[0]
    for k in range(1, parts_ref.shape[0]):
        total = total + parts_ref[k]
    total = total * jnp.float32(scaling)
    own_ref[...] = total
    examples = total.shape[1]
    ids = lax.broadcasted_iota(jnp.int32, (examples, pairs_ref.shape[1]), 0)

    def pick(which):
        chosen = (ids == pairs_ref[which : which + 1, :]).astype(jnp.float32)
        return jnp.dot(total, chosen, precision=lax.Precision.HIGHEST, preferred_element_type=jnp.float32)

    score_ref[...] = jnp.sum(pick(0) * pick(1), axis=0, keepdims=True) * jnp.float32(score_scaling)


def finish(parts, pairs, scaling, score_scaling):
    vmem = pl.BlockSpec(memory_space=pltpu.VMEM)
    return pl.pallas_call(
        functools.partial(finish_kernel, scaling, score_scaling),
        out_shape=(
            jax.ShapeDtypeStruct(parts.shape[1:], jnp.float32),
            jax.ShapeDtypeStruct((1, pairs.shape[1]), jnp.float32),
        ),
        in_specs=[vmem, vmem],
        out_specs=(vmem, vmem),
        compiler_params=pltpu.CompilerParams(vmem_limit_bytes=12 << 20),
        name="finish",
    )(parts, pairs)


def per_device(example_grads, tile_seeds, pair_index):
    examples, params = example_grads.shape
    devices = lax.axis_size("blk")
    col_total = tile_seeds.shape[1] * TILE
    own = col_total // devices
    side = math.isqrt(devices // CORES)
    half = side // 2
    assert side * side * CORES == devices and side * CORES * own == TILE and side % 2 == 0
    me = lax.axis_index("blk").astype(jnp.int32).reshape(1)

    def place(y, x, c):
        return (y * side + x) * CORES + c

    def swap(array, flip):
        return lax.ppermute(array, "blk", [(d, d ^ flip) for d in range(devices)])

    seeds, tables = prepare(me, tile_seeds, side, own)

    alike = [
        [place(2 * i + py, 2 * j + px, c) for i in range(half) for j in range(half)]
        for py in range(2)
        for px in range(2)
        for c in range(CORES)
    ]
    chips = [[place(y, x, c) for y in range(side) for x in range(side)] for c in range(CORES)]
    next_core, next_x, next_y = 1, CORES, CORES * side

    def columns(after, x_flip, y_flip, core_flip):
        return project(after, seeds, tables, example_grads, own, side, (x_flip, y_flip, core_flip))

    both_far = columns(seeds, 1, 1, 1)
    x_far = columns(both_far, 1, 0, 1)
    both = columns(x_far, 1, 1, 0) + swap(both_far, next_core)
    both_in = swap(both, next_x)
    x_own = columns(both, 1, 0, 0) + swap(x_far, next_core)
    x_in = swap(x_own, next_x)
    y_far = columns(x_own, 0, 1, 1)
    y_own = columns(y_far, 0, 1, 0) + swap(y_far, next_core) + both_in
    y_in = swap(y_own, next_y)
    far = columns(y_own, 0, 0, 1)
    same = columns(far, 0, 0, 0) + swap(far, next_core) + x_in + y_in
    parts = lax.all_to_all(same.reshape(half * half, own, examples), "blk", 0, 0, axis_index_groups=alike, tiled=True)
    own_rows, partial = finish(parts, pair_index.T, 1.0 / math.sqrt(params * devices), 1.0 / math.sqrt(col_total))
    partial = partial + swap(partial, next_core)
    spread = jnp.broadcast_to(partial[None], (side * side,) + partial.shape)
    shares = lax.all_to_all(spread, "blk", 0, 0, axis_index_groups=chips, tiled=True)
    scores = jnp.sum(shares, axis=(0, 1))
    return (own_rows, scores)


def solution(mesh):
    placed = (P("grp", "blk"), P("blk", None), P("grp", None))
    return jax.shard_map(
        per_device,
        mesh=mesh,
        in_specs=placed,
        out_specs=(P("blk", "grp"), P("grp")),
        check_vma=False,
    )
```

```python
import functools
import math

import jax
import jax.numpy as jnp
from jax import lax
from jax.experimental import pallas as pl
from jax.experimental.pallas import tpu as pltpu
from jax.sharding import PartitionSpec as P


TILE = 512
PIECE = 16
WIDTH = 256
CORES = 2

golden_mult = -1640531535
mixer_one = -2048144789
mixer_two = -1028477387


def minus_two_bits(table, seed):
    mixed = (table ^ seed) * jnp.int32(mixer_one)
    mixed = mixed ^ lax.shift_right_logical(mixed, jnp.int32(13))
    mixed = mixed * jnp.int32(mixer_two)
    mixed = mixed ^ lax.shift_right_logical(mixed, jnp.int32(16))
    return jnp.where(mixed.astype(jnp.int16) < 0, jnp.bfloat16(-2), jnp.bfloat16(0))


def prepare_kernel(half, side, own, me_ref, seeds_ref, rows_ref, tables_ref):
    tiles = seeds_ref.shape[0]
    me = me_ref[0]
    own_y = (me // (CORES * side)) & 1
    shape = (half * own, TILE)
    row = lax.broadcasted_iota(jnp.int32, shape, 0)
    param = lax.broadcasted_iota(jnp.int32, shape, 1)
    index = param * TILE + (row // own) * (2 * CORES * own) + row % own
    for flip in range(2 * CORES):
        place = (me & (2 * CORES - 1)) ^ flip
        product = (index + place * own) * jnp.int32(golden_mult)
        tables_ref[flip * half * own : (flip + 1) * half * own, :] = product ^ lax.shift_right_logical(product, jnp.int32(16))
    seeds = seeds_ref[...]
    seeds = seeds ^ lax.shift_right_logical(seeds, jnp.int32(16))
    for y in range(2 * half):
        row = pl.multiple_of((((y & 1) ^ own_y) * half + y // 2) * tiles, tiles)
        rows_ref[pl.ds(row, tiles), :] = jnp.broadcast_to(seeds[:, y : y + 1], (tiles, WIDTH))


def prepare(me, seeds, side, own):
    half = side // 2
    vmem = pl.BlockSpec(memory_space=pltpu.VMEM)
    return pl.pallas_call(
        functools.partial(prepare_kernel, half, side, own),
        out_shape=(
            jax.ShapeDtypeStruct((2 * half * seeds.shape[0], WIDTH), jnp.int32),
            jax.ShapeDtypeStruct((2 * CORES * half * own, TILE), jnp.int32),
        ),
        in_specs=[pl.BlockSpec(memory_space=pltpu.SMEM), vmem],
        out_specs=(vmem, vmem),
        compiler_params=pltpu.CompilerParams(vmem_limit_bytes=12 << 20),
        cost_estimate=pl.CostEstimate(flops=1 << 30, bytes_accessed=1 << 16, transcendentals=0),
        name="prepare",
    )(me, seeds)


def project_kernel(own, half, tiles, units, first, after_ref, seeds_ref, tables_ref, grads_ref, *outs):
    del after_ref
    examples = grads_ref.shape[0]
    tile_rows = half * own
    pieces = half * tile_rows // PIECE
    parts = TILE // WIDTH

    def run(*sums):
        acc = [sums[part * (pieces + 1) : (part + 1) * (pieces + 1)] for part in range(parts)]
        if first:
            for one in sums:
                pltpu.matmul_pop(one)

        def push(tile):
            for part in range(parts):
                block = grads_ref[:, pl.ds(pl.multiple_of(tile * TILE + part * WIDTH, WIDTH), WIDTH)]
                block = jnp.concatenate([block, jnp.zeros((WIDTH - examples, WIDTH), block.dtype)], axis=0)
                pltpu.matmul_push_rhs(block, staging_register=0, mxu_index=part, transpose=True)

        push(0)
        for number, (x_flip, y_flip, core_flip) in enumerate(units):
            place = x_flip * CORES + core_flip
            table = tables_ref.at[place * tile_rows : (place + 1) * tile_rows, :]

            def tile_step(tile, following):
                for part in range(parts):
                    pltpu.matmul_acc_lhs(acc[part][pieces], jnp.ones((PIECE, WIDTH), jnp.bfloat16), load_staged_rhs=0)
                if following is not None:
                    push(following)
                for i in range(half):
                    seed = seeds_ref[pl.ds((y_flip * half + i) * tiles + tile, 1), :]
                    for start in range(0, tile_rows, PIECE):
                        for part in range(parts):
                            pltpu.matmul_acc_lhs(
                                acc[part][(i * tile_rows + start) // PIECE],
                                minus_two_bits(table[start : start + PIECE, part * WIDTH : (part + 1) * WIDTH], seed),
                            )

            def pair_step(pair, carry):
                tile_step(2 * pair, 2 * pair + 1)
                tile_step(2 * pair + 1, 2 * pair + 2)
                return carry

            lax.fori_loop(0, tiles // 2 - 1, pair_step, 0)
            tile_step(tiles - 2, tiles - 1)
            tile_step(tiles - 1, 0 if number + 1 < len(units) else None)
            whole = sum(pltpu.matmul_pop(acc[part][pieces])[:, :examples] for part in range(parts))
            for piece in range(pieces):
                total = sum(pltpu.matmul_pop(acc[part][piece])[:, :examples] for part in range(parts))
                if len(outs) == len(units):
                    outs[number][piece * PIECE : (piece + 1) * PIECE, :] = whole + total
                else:
                    row = (number * pieces + piece) * PIECE
                    outs[0][row : row + PIECE, :] = whole + total

    pl.run_scoped(run, *[pltpu.ACC(part)((PIECE, WIDTH), jnp.float32) for part in range(parts) for _ in range(pieces + 1)])


def project(after, seeds, tables, grads, own, side, units, outputs):
    examples, params = grads.shape
    half = side // 2
    rows = half * half * own
    vmem = pl.BlockSpec(memory_space=pltpu.VMEM)
    return pl.pallas_call(
        functools.partial(project_kernel, own, half, params // TILE, units, after is seeds),
        out_shape=(jax.ShapeDtypeStruct((len(units) // outputs * rows, examples), jnp.float32),) * outputs,
        in_specs=[vmem] * 4,
        out_specs=(vmem,) * outputs,
        compiler_params=pltpu.CompilerParams(vmem_limit_bytes=12 << 20),
        cost_estimate=pl.CostEstimate(
            flops=8 * len(units) * rows * examples * params, bytes_accessed=2 * examples * params, transcendentals=0
        ),
        name="project",
    )(after, seeds, tables, grads)


def finish_kernel(scaling, score_scaling, parts_ref, pairs_ref, own_ref, score_ref):
    total = parts_ref[0]
    for k in range(1, parts_ref.shape[0]):
        total = total + parts_ref[k]
    own_ref[...] = total
    total = total * jnp.float32(scaling)
    examples = total.shape[1]
    ids = lax.broadcasted_iota(jnp.int32, (examples, pairs_ref.shape[1]), 0)

    def pick(which):
        chosen = (ids == pairs_ref[which : which + 1, :]).astype(jnp.float32)
        return jnp.dot(total, chosen, precision=lax.Precision.HIGHEST, preferred_element_type=jnp.float32)

    score_ref[...] = jnp.sum(pick(0) * pick(1), axis=0, keepdims=True) * jnp.float32(score_scaling)


def finish(parts, pairs, scaling, score_scaling):
    vmem = pl.BlockSpec(memory_space=pltpu.VMEM)
    return pl.pallas_call(
        functools.partial(finish_kernel, scaling, score_scaling),
        out_shape=(
            jax.ShapeDtypeStruct(parts.shape[1:], jnp.float32),
            jax.ShapeDtypeStruct((1, pairs.shape[1]), jnp.float32),
        ),
        in_specs=[vmem, vmem],
        out_specs=(vmem, vmem),
        compiler_params=pltpu.CompilerParams(vmem_limit_bytes=12 << 20),
        name="finish",
    )(parts, pairs)


def per_device(example_grads, tile_seeds, pair_index):
    examples, params = example_grads.shape
    devices = lax.axis_size("blk")
    col_total = tile_seeds.shape[1] * TILE
    own = col_total // devices
    side = math.isqrt(devices // CORES)
    half = side // 2
    assert side * side * CORES == devices and side * CORES * own == TILE and side % 2 == 0
    me = lax.axis_index("blk").astype(jnp.int32).reshape(1)

    def place(y, x, c):
        return (y * side + x) * CORES + c

    def swap(array, flip):
        return lax.ppermute(array, "blk", [(d, d ^ flip) for d in range(devices)])

    seeds, tables = prepare(me, tile_seeds, side, own)

    alike = [
        [place(2 * i + py, 2 * j + px, c) for i in range(half) for j in range(half)]
        for py in range(2)
        for px in range(2)
        for c in range(CORES)
    ]
    chips = [sum((group for group in alike if group[0] % CORES == c), []) for c in range(CORES)]
    next_core, next_x, next_y = 1, CORES, CORES * side

    def columns(after, *units, outputs=1):
        return project(after, seeds, tables, example_grads, own, side, units, outputs)

    (x_far,) = columns(seeds, (1, 1, 1), (1, 0, 1))
    (both,) = columns(x_far, (1, 1, 0))
    x_core = swap(x_far, next_core)
    both = both + x_core[: both.shape[0]]
    both_in = swap(both, next_x)
    x_own, y_far = columns(both, (1, 0, 0), (0, 1, 1), outputs=2)
    x_own = x_own + x_core[both.shape[0] :]
    x_in = swap(x_own, next_x)
    (y_own,) = columns(x_own, (0, 1, 0))
    y_own = y_own + swap(y_far, next_core) + both_in
    y_in = swap(y_own, next_y)
    (far,) = columns(y_own, (0, 0, 1))
    (same,) = columns(far, (0, 0, 0))
    same = same + swap(far, next_core) + x_in + y_in
    parts = lax.all_to_all(same.reshape(half * half, own, examples), "blk", 0, 0, axis_index_groups=alike, tiled=True)
    scaling = 1.0 / math.sqrt(params * devices)
    own_rows, partial = finish(parts, pair_index.T, scaling, 1.0 / math.sqrt(col_total))
    partial = partial + swap(partial, next_core)
    own_rows = own_rows * scaling
    spread = jnp.broadcast_to(partial[None], (side * side,) + partial.shape)
    shares = lax.all_to_all(spread, "blk", 0, 0, axis_index_groups=chips, tiled=True)
    scores = jnp.sum(shares, axis=(0, 1))
    return (own_rows, scores)


def solution(mesh):
    placed = (P("grp", "blk"), P("blk", None), P("grp", None))
    return jax.shard_map(
        per_device,
        mesh=mesh,
        in_specs=placed,
        out_specs=(P("blk", "grp"), P("grp")),
        check_vma=False,
    )
```
